32 devices in a mesh: ep: 4 (over z), tp: 8 (over y, x, core).
Axes of the slice: x: 2, y: 2, z: 4, core: 2. Of those that a mesh axis runs over, the one named last changes fastest.
Arguments:
- tokens: bfloat16 [384, 3072], P('ep', 'tp'), may hold values from -6 to 6
- cotangent: bfloat16 [384, 3072], P('ep', 'tp'), may hold values from -6 to 6
- expert_ids: int32 [384, 2], P('ep'), may hold values from 0 to 3, all different within a row; in each aligned block of 96 rows (0 to 95, 96 to 191, ...) at most 80 rows name the same one
- combine_weights: float32 [384, 2], P('ep'), may hold values from 0.1 to 1
- w_gate: bfloat16 [4, 3072, 8192], P('ep', None, 'tp'), may hold values from -0.15625 to 0.15625
- w_up: bfloat16 [4, 3072, 8192], P('ep', None, 'tp'), may hold values from -0.109375 to 0.109375
- w_down: bfloat16 [4, 8192, 3072], P('ep', 'tp'), may hold values from -0.09375 to 0.09375
Outputs:
- mixed: bfloat16 [384, 3072], P('ep', 'tp')
- grad_tokens: bfloat16 [384, 3072], P('ep', 'tp')
- grad_combine: float32 [384, 2], P('ep')
- grad_gate: bfloat16 [4, 3072, 8192], P('ep', 'tp')
- grad_up: bfloat16 [4, 3072, 8192], P('ep', 'tp')
- grad_down: bfloat16 [4, 8192, 3072], P('ep', None, 'tp')
The draws below stay inside these ranges and needn't reach their ends.
Inputs may be any that keep to these rules, and one draw needn't show every extreme that they name: `expert_ids`: each row names 2 different experts. Among the 96 rows of one index of ep, no expert is named more than 80 times, and in some such blocks one expert is named exactly 80 times.
All inputs are finite; a program needn't handle non-finite values.
Results may differ from the reference program's by a relative error of at most 0.019.
Values may be sent and summed in bfloat16 or wider, within the bound.
A program may use at most 128 MiB of HBM per device.

```python
import math
import jax
import jax.numpy as jnp
import numpy as np
from jax import lax

D = 3072
FF = 8192
TOP = 2
TOK_EP = 96
EXPERTS = 4
CAP = 80
TOKENS = 384
N_EP = 4
N_TP = 8


def with_spikes(drawn, stream_key, source, target, parts, factor):
    def block_of(axis_at):
        return (jnp.arange(drawn.shape[axis_at]) // (drawn.shape[axis_at] // parts)).reshape((-1,) + (1,) * (drawn.ndim - 1 - axis_at))

    first = jax.random.permutation(stream_key, parts)[block_of(target)]
    other_side = (block_of(target) + parts // 2) % parts
    return jnp.where((block_of(source) == first) | (block_of(source) == other_side), factor * drawn, drawn)


def level_of(stream_key, shape, shards, least, largest):
    def one(position, parts):
        draws = jax.random.uniform(jax.random.fold_in(jax.random.fold_in(stream_key, 6), position), (parts,), jnp.float32, least / len(shards), largest / len(shards))
        return jnp.repeat(jnp.exp(draws), shape[position] // parts).reshape((-1,) + (1,) * (len(shape) - position - 1))

    loudness = one(*shards[0])
    for cut in shards[1:]:
        loudness = loudness * one(*cut)
    return loudness


def assign_block(key, own, number, rows, amount, top, most, skew):
    ranking = jax.random.permutation(key, amount)
    packed, usual = shares(amount, rows * top, most, skew, True), shares(amount, rows * top, most, skew, False)
    places = jnp.arange(amount)

    def named(tallies, rotation):
        used = int((tallies > 0).sum())
        fixed = max(1, used // 4)
        passed = fixed + (places - fixed + rotation * (used - fixed)) % max(1, amount - fixed)
        return jnp.zeros((amount,), jnp.int32).at[ranking[jnp.where(places < fixed, places, passed)]].set(jnp.asarray(tallies, jnp.int32))

    tallies = jnp.where(number % 4 == 0, named(packed, number // 4), named(usual, number - number // 4 - 1))
    mixed = jax.random.permutation(jax.random.fold_in(own, 3), amount)
    giver, receiver = mixed[0:amount // 2 * 2:2], mixed[1:amount // 2 * 2:2]
    margin = jnp.minimum(tallies[giver] - 1, most - tallies[receiver]) // 2
    margin = jnp.where((giver == ranking[0]) | (receiver == ranking[0]) | (tallies[receiver] == 0), 0, jnp.maximum(margin, 0))
    passed = jax.random.randint(jax.random.fold_in(own, 4), (amount // 2,), 0, 1 << 20) % (margin + 1)
    tallies = tallies.at[giver].add(-passed).at[receiver].add(passed)
    members = jnp.searchsorted(jnp.cumsum(tallies), jnp.arange(rows * top), side="right").astype(jnp.int32)
    grid = members.reshape(top, rows).T
    grid = grid[jax.random.permutation(jax.random.fold_in(own, 1), rows)]
    rotation = jax.random.randint(jax.random.fold_in(own, 2), (rows, 1), 0, top)
    return jnp.take_along_axis(grid, (jnp.arange(top)[None, :] + rotation) % top, axis=1)


def shares(count, total, bound, lean, full):
    portions = [(1 << 20) // math.isqrt(standing ** lean) + 1 for standing in range(1, count + 1)]
    largest = bound if full else min(bound, max(-(-total // count), total * portions[0] // sum(portions)))
    least = 1 if total - largest >= count - 1 else 0
    given, spare = [largest] + [least] * (count - 1), total - largest - least * (count - 1)
    while spare > 0:
        candidates = [i for i in range(1, count) if given[i] < largest] or [i for i in range(1, count) if given[i] < bound]
        mass, left = sum([portions[i] for i in candidates]), spare
        for i in candidates:
            extra = min(bound - given[i], max(1, left * portions[i] // mass), spare)
            given[i] = given[i] + extra
            spare = spare - extra
    return np.array(given)


def noise(key, extent, scale, limit, cuts=(), held_as=jnp.bfloat16):
    result = scale * jax.random.normal(key, extent, jnp.float32)
    if cuts:
        result = result * level_of(key, extent, cuts, -0.22, 0.18)
    return jnp.clip(result, -limit, limit).astype(held_as)


def heavy_noise(own_key, dims, spread, bound, shards, heavy, kind=jnp.bfloat16):
    values = spread * jax.random.normal(own_key, dims, jnp.float32)
    if shards:
        values = values * level_of(own_key, dims, shards, -0.22, 0.18)
    return jnp.clip(with_spikes(values, jax.random.fold_in(own_key, 3), *heavy), -bound, bound).astype(kind)


def setup_inputs(seed: int = 0) -> dict:
    key_of = jax.random.split(jax.random.key(seed), 8)
    tokens = noise(key_of[0], (TOKENS, D), 1.0, 6.0, ((0, 4), (1, 8)))
    cotangent = noise(key_of[1], (TOKENS, D), 1.0, 6.0, ((0, 4), (1, 8)))
    expert_ids_keys = jax.random.split(jax.random.fold_in(key_of[2], 1), TOKENS // TOK_EP)
    expert_ids_turns = jax.random.permutation(jax.random.fold_in(key_of[2], 3), TOKENS // TOK_EP)
    expert_ids = jax.vmap(lambda own, number: assign_block(jax.random.fold_in(key_of[2], 2), own, number, TOK_EP, N_EP, TOP, CAP, 2))(expert_ids_keys, expert_ids_turns).reshape((TOKENS, TOP))
    combine_weights = jnp.clip(jnp.exp(math.log(1.0) - 2.3025851 * jax.random.uniform(key_of[3], (TOKENS, TOP), jnp.float32) ** level_of(key_of[3], (TOKENS, TOP), ((0, 4),), -0.2, 0.2)), 0.1, 1.0)
    w_gate = heavy_noise(key_of[4], (EXPERTS, D, FF), D ** -0.5, 0.15625, ((0, 4), (2, 8)), (2, 1, 8, 2.0))
    w_up = noise(key_of[5], (EXPERTS, D, FF), D ** -0.5, 0.109375, ((0, 4), (2, 8)))
    w_down = heavy_noise(key_of[6], (EXPERTS, FF, D), FF ** -0.5, 0.09375, ((0, 4), (1, 8)), (1, 2, 8, 2.0))
    return {"tokens": tokens, "cotangent": cotangent, "expert_ids": expert_ids, "combine_weights": combine_weights, "w_gate": w_gate, "w_up": w_up, "w_down": w_down}


def silu_parts(gate_pre):
    sigma = jax.nn.sigmoid(gate_pre)
    return gate_pre * sigma, sigma * (1.0 + gate_pre * (1.0 - sigma))


def slot_rows(expert_ids):
    groups = expert_ids.reshape(N_EP, TOK_EP * TOP)
    onehot = (groups[:, :, None] == jnp.arange(N_EP, dtype=jnp.int32)[None, None, :]).astype(jnp.int32)
    before = jnp.cumsum(onehot, axis=1) - onehot
    rank = jnp.sum(before * onehot, axis=2)
    source = jnp.arange(N_EP, dtype=jnp.int32)[:, None]
    return (source * CAP + rank).reshape(-1).astype(jnp.int32)


def rounded_blocks(pairs, rows):
    width = FF // N_TP

    def step(total, index):
        start = index * width
        part = jnp.zeros((rows, D), jnp.float32)
        for left, right in pairs:
            left_block = lax.dynamic_slice_in_dim(left, start, width, 1)
            right_block = lax.dynamic_slice_in_dim(right, start, width, 0)
            part = part + jnp.dot(left_block, right_block, preferred_element_type=jnp.float32)
        rounded = lax.optimization_barrier(part.astype(jnp.bfloat16))
        return total + rounded.astype(jnp.float32), None

    total, _ = lax.scan(step, jnp.zeros((rows, D), jnp.float32), jnp.arange(N_TP, dtype=jnp.int32))
    return total.astype(jnp.bfloat16)


def reference(tokens, cotangent, expert_ids, combine_weights, w_gate, w_up, w_down):
    flat_ids = expert_ids.reshape(-1)
    rows = slot_rows(expert_ids)
    owner = jnp.repeat(jnp.arange(TOKENS, dtype=jnp.int32), TOP)
    weight_flat = combine_weights.reshape(-1)
    buffer_rows = N_EP * CAP
    x_buffer = jnp.zeros((N_EP, buffer_rows, D), jnp.bfloat16).at[flat_ids, rows].set(tokens[owner])
    grad_out = (weight_flat[:, None] * cotangent[owner].astype(jnp.float32)).astype(jnp.bfloat16)
    dy_buffer = jnp.zeros((N_EP, buffer_rows, D), jnp.bfloat16).at[flat_ids, rows].set(grad_out)
    outs_list, ins_list, gates_list, ups_list, downs_list = [], [], [], [], []
    for expert in range(N_EP):
        x_rows = x_buffer[expert]
        dy_rows = dy_buffer[expert]
        gate_pre = jnp.dot(x_rows, w_gate[expert], preferred_element_type=jnp.float32)
        up_pre = jnp.dot(x_rows, w_up[expert], preferred_element_type=jnp.float32)
        active, slope = silu_parts(gate_pre)
        hidden = (active * up_pre).astype(jnp.bfloat16)
        outs_list.append(rounded_blocks([(hidden, w_down[expert])], buffer_rows))
        grad_hidden = jnp.dot(dy_rows, w_down[expert].T, preferred_element_type=jnp.float32)
        grad_gate_pre = (grad_hidden * up_pre * slope).astype(jnp.bfloat16)
        grad_up_pre = (grad_hidden * active).astype(jnp.bfloat16)
        ins_list.append(rounded_blocks([(grad_gate_pre, w_gate[expert].T), (grad_up_pre, w_up[expert].T)], buffer_rows))
        gates_list.append(jnp.dot(x_rows.T, grad_gate_pre, preferred_element_type=jnp.float32).astype(jnp.bfloat16))
        ups_list.append(jnp.dot(x_rows.T, grad_up_pre, preferred_element_type=jnp.float32).astype(jnp.bfloat16))
        downs_list.append(jnp.dot(hidden.T, dy_rows, preferred_element_type=jnp.float32).astype(jnp.bfloat16))
    expert_out = jnp.stack(outs_list)[flat_ids, rows].reshape(TOKENS, TOP, D).astype(jnp.float32)
    grad_in = jnp.stack(ins_list)[flat_ids, rows].reshape(TOKENS, TOP, D).astype(jnp.float32)
    mixed = jnp.sum(combine_weights[:, :, None] * expert_out, axis=1).astype(jnp.bfloat16)
    grad_combine = jnp.sum(cotangent.astype(jnp.float32)[:, None, :] * expert_out, axis=2)
    grad_tokens = jnp.sum(grad_in, axis=1).astype(jnp.bfloat16)
    return (mixed, grad_tokens, grad_combine, jnp.stack(gates_list), jnp.stack(ups_list), jnp.stack(downs_list))
```

```python
import jax
import jax.numpy as jnp
from jax import lax
from jax.sharding import PartitionSpec as P


def silu_parts(gate_pre):
    sigma = jax.nn.sigmoid(gate_pre)
    return (gate_pre * sigma, sigma * (1.0 + gate_pre * (1.0 - sigma)))


def contract_rows(left, right):
    return lax.dot_general(
        left, right, (((0,), (0,)), ((), ())), preferred_element_type=jnp.float32
    )


def contract_cols(left, right):
    return lax.dot_general(
        left, right, (((1,), (1,)), ((), ())), preferred_element_type=jnp.float32
    )


def body(tokens, cotangent, expert_ids, combine_weights, w_gate, w_up, w_down):
    groups = lax.axis_size("ep")
    tok_rows, piece_width = tokens.shape
    chosen = expert_ids.shape[1]
    capacity = tok_rows * chosen * 5 // (3 * groups)
    buffer_rows = groups * capacity
    gate_weight = w_gate[0]
    up_weight = w_up[0]
    down_weight = w_down[0]
    flat_ids = expert_ids.reshape(-1)
    onehot = (flat_ids[:, None] == jnp.arange(groups, dtype=jnp.int32)[None, :]).astype(jnp.int32)
    rank = jnp.sum((jnp.cumsum(onehot, axis=0) - onehot) * onehot, axis=1)
    slot_index = flat_ids * capacity + rank
    places = (jnp.arange(buffer_rows, dtype=jnp.int32)[:, None] == slot_index[None, :]).astype(
        jnp.bfloat16
    )
    placer = jnp.sum(
        places.reshape(buffer_rows, tok_rows, chosen).astype(jnp.float32), axis=2
    ).astype(jnp.bfloat16)
    scaled = (combine_weights[:, :, None] * cotangent[:, None, :].astype(jnp.float32)).astype(
        jnp.bfloat16
    )
    send_grad = jnp.dot(
        places, scaled.reshape(tok_rows * chosen, piece_width), preferred_element_type=jnp.float32
    ).astype(jnp.bfloat16)
    send_rows = jnp.dot(placer, tokens, preferred_element_type=jnp.float32).astype(jnp.bfloat16)
    recv_rows, recv_grad = (
        lax.all_to_all(
            send_rows.reshape(groups, capacity, piece_width),
            "ep",
            split_axis=0,
            concat_axis=0,
            tiled=True,
        ),
        lax.all_to_all(
            send_grad.reshape(groups, capacity, piece_width),
            "ep",
            split_axis=0,
            concat_axis=0,
            tiled=True,
        ),
    )
    recv_rows = recv_rows.reshape(buffer_rows, piece_width)
    piece = lax.all_gather(recv_rows, "tp", axis=1, tiled=True)
    gate_pre = jnp.dot(piece, gate_weight, preferred_element_type=jnp.float32)
    up_pre = jnp.dot(piece, up_weight, preferred_element_type=jnp.float32)
    recv_grad = recv_grad.reshape(buffer_rows, piece_width)
    active, slope = silu_parts(gate_pre)
    hidden = (active * up_pre).astype(jnp.bfloat16)
    partial_value = jnp.dot(hidden, down_weight, preferred_element_type=jnp.float32)
    out_piece = lax.psum_scatter(
        partial_value.astype(jnp.bfloat16), "tp", scatter_dimension=1, tiled=True
    )
    out_back = lax.all_to_all(
        out_piece.reshape(groups, capacity, piece_width),
        "ep",
        split_axis=0,
        concat_axis=0,
        tiled=True,
    ).reshape(buffer_rows, piece_width)
    out_tokens = (
        jnp.take(out_back, slot_index, axis=0)
        .reshape(tok_rows, chosen, piece_width)
        .astype(jnp.float32)
    )
    mixed = jnp.sum(combine_weights[:, :, None] * out_tokens, axis=1).astype(jnp.bfloat16)
    local_products = jnp.sum(cotangent.astype(jnp.float32)[:, None, :] * out_tokens, axis=2)
    grad_combine = lax.psum(local_products, "tp")
    grad_hidden = contract_cols(lax.all_gather(recv_grad, "tp", axis=1, tiled=True), down_weight)
    grad_gate_pre = (grad_hidden * up_pre * slope).astype(jnp.bfloat16)
    grad_up_pre = (grad_hidden * active).astype(jnp.bfloat16)
    input_partial = contract_cols(grad_gate_pre, gate_weight) + contract_cols(
        grad_up_pre, up_weight
    )
    input_piece = lax.psum_scatter(
        input_partial.astype(jnp.bfloat16), "tp", scatter_dimension=1, tiled=True
    )
    input_back = lax.all_to_all(
        input_piece.reshape(groups, capacity, piece_width),
        "ep",
        split_axis=0,
        concat_axis=0,
        tiled=True,
    ).reshape(buffer_rows, piece_width)
    grad_tokens = jnp.sum(
        jnp.take(input_back, slot_index, axis=0)
        .reshape(tok_rows, chosen, piece_width)
        .astype(jnp.float32),
        axis=1,
    ).astype(jnp.bfloat16)
    down_cols_out = contract_rows(
        lax.all_gather(hidden, "tp", axis=1, tiled=True), recv_grad
    ).astype(jnp.bfloat16)
    gate_rows_out = contract_rows(
        recv_rows, lax.all_gather(grad_gate_pre, "tp", axis=1, tiled=True)
    ).astype(jnp.bfloat16)
    up_rows_out = contract_rows(
        recv_rows, lax.all_gather(grad_up_pre, "tp", axis=1, tiled=True)
    ).astype(jnp.bfloat16)
    return (
        mixed,
        grad_tokens,
        grad_combine,
        gate_rows_out[None],
        up_rows_out[None],
        down_cols_out[None],
    )


def solution(mesh):
    placed = (
        P("ep", "tp"),
        P("ep", "tp"),
        P("ep", None),
        P("ep", None),
        P("ep", None, "tp"),
        P("ep", None, "tp"),
        P("ep", "tp", None),
    )
    return jax.shard_map(
        body,
        mesh=mesh,
        in_specs=placed,
        out_specs=(
            P("ep", "tp"),
            P("ep", "tp"),
            P("ep", None),
            P("ep", "tp", None),
            P("ep", "tp", None),
            P("ep", None, "tp"),
        ),
        check_vma=False,
    )
```

```python
import functools
import math

import jax
import jax.numpy as jnp
from jax import lax
from jax.experimental import pallas as pl
from jax.experimental.pallas import tpu as pltpu
from jax.sharding import PartitionSpec as P

MESH = pl.DeviceIdType.MESH
BF = jnp.bfloat16


def ring_order(chips):
    side_x = math.isqrt(chips)
    side_x = side_x if side_x * side_x == chips else chips // 2
    side_y = chips // side_x
    order = [x for x in range(side_x)]
    for y in range(1, side_y):
        xs = range(side_x - 1, 0, -1) if y % 2 else range(1, side_x)
        order += [y * side_x + x for x in xs]
    order += [y * side_x for y in range(side_y - 1, 0, -1)]
    return order


def pick(table, index):
    value = jnp.int32(table[0])
    for i in range(1, len(table)):
        value = jnp.where(index == i, jnp.int32(table[i]), value)
    return value


def remote(src, dst, send, recv, device):
    return pltpu.make_async_remote_copy(
        src_ref=src,
        dst_ref=dst,
        send_sem=send,
        recv_sem=recv,
        device_id={"tp": device},
        device_id_type=MESH,
    )


def greet(devices):
    barrier = pltpu.get_barrier_semaphore()
    for device in devices:
        pl.semaphore_signal(barrier, inc=1, device_id={"tp": device}, device_id_type=MESH)
    pl.semaphore_wait(barrier, len(devices))


def gather_kernel(count, chips, *refs):
    own, out = refs[:count], refs[count : 2 * count]
    ring_send, ring_recv, core_send, core_recv, keep = refs[2 * count :]
    order = ring_order(chips)
    place = [order.index(chip) for chip in range(chips)]
    me = lax.axis_index("tp")
    chip, core = me // 2, me % 2
    spot = pick(place, chip)
    partner = chip * 2 + 1 - core
    steps = chips // 2
    rows = own[0].shape[0]
    half = rows // 2

    def at(offset):
        return pick(order, (spot + offset + chips) % chips) * 2 + core

    right, left = at(1), at(-1)
    greet([right, left, partner])

    def part(ref, way, step):
        if step < steps - 1:
            return ref
        return ref.at[pl.ds(way * half, half)]

    def hop(k, way, step):
        index = at(-step if way == 0 else step)
        source = own[k] if step == 0 else out[k].at[index]
        return remote(
            part(source, way, step),
            part(out[k].at[index], way, step),
            ring_send.at[k, way, step],
            ring_recv.at[k, way, step],
            right if way == 0 else left,
        )

    def arrived(k, way, step):
        index = at(-(step + 1) if way == 0 else step + 1)
        block = part(out[k].at[index], way, step)
        return remote(
            block, block, ring_send.at[k, way, step], ring_recv.at[k, way, step], right if way == 0 else left
        ), remote(
            block, block, core_send.at[k, way, step], core_recv.at[k, way, step], partner
        )

    def own_pass(k):
        return remote(
            own[k], out[k].at[me], core_send.at[k, 2, 0], core_recv.at[k, 2, 0], partner
        )

    def own_keep(k):
        return pltpu.make_async_copy(own[k], out[k].at[me], keep.at[k])

    for k in range(count):
        for way in range(2):
            hop(k, way, 0).start()
    for k in range(count):
        own_pass(k).start()
        own_keep(k).start()
    for step in range(steps):
        for k in range(count):
            for way in range(2):
                landed, handed = arrived(k, way, step)
                landed.wait_recv()
                if step + 1 < steps:
                    hop(k, way, step + 1).start()
                handed.start()
    for k in range(count):
        own_keep(k).wait()
        own_pass(k).wait_send()
        other = remote(
            own[k], out[k].at[partner], core_send.at[k, 2, 0], core_recv.at[k, 2, 0], partner
        )
        other.wait_recv()
        for way in range(2):
            for step in range(steps):
                hop(k, way, step).wait_send()
                handed = arrived(k, way, step)[1]
                handed.wait_send()
                index = at(-(step + 1) if way == 0 else step + 1) // 2 * 2 + 1 - core
                block = part(out[k].at[index], way, step)
                remote(
                    block, block, core_send.at[k, way, step], core_recv.at[k, way, step], partner
                ).wait_recv()


def gather(arrays, ident):
    size = lax.axis_size("tp")
    chips, count = size // 2, len(arrays)
    ring = pltpu.SemaphoreType.DMA((count, 2, chips // 2))
    cores = pltpu.SemaphoreType.DMA((count, 3, chips // 2))
    return pl.pallas_call(
        functools.partial(gather_kernel, count, chips),
        out_shape=[jax.ShapeDtypeStruct((size,) + a.shape, a.dtype) for a in arrays],
        in_specs=[pl.BlockSpec(memory_space=pltpu.VMEM)] * count,
        out_specs=[pl.BlockSpec(memory_space=pl.ANY)] * count,
        scratch_shapes=[ring, ring, cores, cores, pltpu.SemaphoreType.DMA((count,))],
        compiler_params=pltpu.CompilerParams(collective_id=ident, has_side_effects=True),
        name=f"gather_{ident}",
    )(*arrays)


def reduce_kernel(count, chips, *refs):
    part, out = refs[:count], refs[count : 2 * count]
    pre, stage, got = refs[2 * count : 5 * count : 3], refs[2 * count + 1 : 5 * count : 3], refs[2 * count + 2 : 5 * count : 3]
    core_send, core_recv, chip_send, chip_recv = refs[5 * count :]
    me = lax.axis_index("tp")
    chip, core = me // 2, me % 2
    partner = chip * 2 + 1 - core
    away = [(chip + o) % chips for o in range(1, chips)]
    greet([partner] + [other * 2 + core for other in away])

    def swap(k):
        return remote(part[k].at[1 - core], pre[k], core_send.at[k], core_recv.at[k], partner)

    def ship(k, o):
        return remote(
            stage[k].at[away[o]], got[k].at[o], chip_send.at[k, o], chip_recv.at[k, o], away[o] * 2 + core
        )

    for k in range(count):
        swap(k).start()
    for k in range(count):
        swap(k).wait()

        def add(q, _):
            stage[k][q] = (
                part[k][core, q].astype(jnp.float32) + pre[k][q].astype(jnp.float32)
            ).astype(BF)
            return 0

        lax.fori_loop(0, chips, add, 0)
        for o in range(chips - 1):
            ship(k, o).start()
    for k in range(count):
        for o in range(chips - 1):
            ship(k, o).wait()
        total = stage[k][chip].astype(jnp.float32)
        for o in range(chips - 1):
            total = total + got[k][o].astype(jnp.float32)
        out[k][...] = total.astype(BF)


def reduce_pieces(partials, ident):
    size = lax.axis_size("tp")
    chips, count = size // 2, len(partials)
    rows, width = partials[0].shape[0], partials[0].shape[1] // size
    cut = [p.reshape(rows, chips, 2, width).transpose(2, 1, 0, 3) for p in partials]
    held = pltpu.VMEM((chips, rows, width), BF)
    got = pltpu.VMEM((chips - 1, rows, width), BF)
    return pl.pallas_call(
        functools.partial(reduce_kernel, count, chips),
        out_shape=[jax.ShapeDtypeStruct((rows, width), BF)] * count,
        in_specs=[pl.BlockSpec(memory_space=pltpu.VMEM)] * count,
        out_specs=[pl.BlockSpec(memory_space=pltpu.VMEM)] * count,
        scratch_shapes=[held, held, got] * count
        + [pltpu.SemaphoreType.DMA((count,))] * 2
        + [pltpu.SemaphoreType.DMA((count, chips - 1))] * 2,
        compiler_params=pltpu.CompilerParams(
            collective_id=ident, has_side_effects=True, vmem_limit_bytes=48 << 20
        ),
        name=f"reduce_{ident}",
    )(*cut)


def rows_kernel(x_ref, g_ref, o_ref):
    o_ref[...] = jnp.dot(x_ref[...], g_ref[0], preferred_element_type=jnp.float32).astype(BF)


def row_grads(x_turned, blocks):
    features, rows = x_turned.shape
    size, _, hidden = blocks.shape
    return pl.pallas_call(
        rows_kernel,
        grid=(size,),
        out_shape=jax.ShapeDtypeStruct((features, size * hidden), BF),
        in_specs=[
            pl.BlockSpec((features, rows), lambda n: (0, 0)),
            pl.BlockSpec((1, rows, hidden), lambda n: (n, 0, 0)),
        ],
        out_specs=pl.BlockSpec((features, hidden), lambda n: (0, n)),
        name="row_grads",
        cost_estimate=pl.CostEstimate(
            flops=2 * features * rows * size * hidden,
            bytes_accessed=2 * size * hidden * (rows + features),
            transcendentals=0,
        ),
    )(x_turned, blocks)


def side_by_side(blocks):
    size, rows, width = blocks.shape
    return blocks.transpose(1, 0, 2).reshape(rows, size * width)


def silu_parts(gate_pre):
    sigma = jax.nn.sigmoid(gate_pre)
    return (gate_pre * sigma, sigma * (1.0 + gate_pre * (1.0 - sigma)))


def contract_rows(left, right):
    return lax.dot_general(
        left, right, (((0,), (0,)), ((), ())), preferred_element_type=jnp.float32
    )


def contract_cols(left, right):
    return lax.dot_general(
        left, right, (((1,), (1,)), ((), ())), preferred_element_type=jnp.float32
    )


def body(tokens, cotangent, expert_ids, combine_weights, w_gate, w_up, w_down):
    groups = lax.axis_size("ep")
    tok_rows, piece_width = tokens.shape
    chosen = expert_ids.shape[1]
    capacity = tok_rows * chosen * 5 // (3 * groups)
    buffer_rows = groups * capacity
    gate_weight = w_gate[0]
    up_weight = w_up[0]
    down_weight = w_down[0]
    flat_ids = expert_ids.reshape(-1)
    onehot = (flat_ids[:, None] == jnp.arange(groups, dtype=jnp.int32)[None, :]).astype(jnp.int32)
    rank = jnp.sum((jnp.cumsum(onehot, axis=0) - onehot) * onehot, axis=1)
    slot_index = flat_ids * capacity + rank
    places = (jnp.arange(buffer_rows, dtype=jnp.int32)[:, None] == slot_index[None, :]).astype(
        jnp.bfloat16
    )
    placer = jnp.sum(
        places.reshape(buffer_rows, tok_rows, chosen).astype(jnp.float32), axis=2
    ).astype(jnp.bfloat16)
    scaled = (combine_weights[:, :, None] * cotangent[:, None, :].astype(jnp.float32)).astype(
        jnp.bfloat16
    )
    send_grad = jnp.dot(
        places, scaled.reshape(tok_rows * chosen, piece_width), preferred_element_type=jnp.float32
    ).astype(jnp.bfloat16)
    send_rows = jnp.dot(placer, tokens, preferred_element_type=jnp.float32).astype(jnp.bfloat16)
    recv_rows, recv_grad = (
        lax.all_to_all(
            send_rows.reshape(groups, capacity, piece_width),
            "ep",
            split_axis=0,
            concat_axis=0,
            tiled=True,
        ),
        lax.all_to_all(
            send_grad.reshape(groups, capacity, piece_width),
            "ep",
            split_axis=0,
            concat_axis=0,
            tiled=True,
        ),
    )
    recv_rows = recv_rows.reshape(buffer_rows, piece_width)
    recv_grad = recv_grad.reshape(buffer_rows, piece_width)
    x_blocks, dy_blocks = gather([recv_rows, recv_grad], 0)
    piece, dy_full = side_by_side(x_blocks), side_by_side(dy_blocks)
    gate_pre = jnp.dot(piece, gate_weight, preferred_element_type=jnp.float32)
    up_pre = jnp.dot(piece, up_weight, preferred_element_type=jnp.float32)
    active, slope = silu_parts(gate_pre)
    hidden = (active * up_pre).astype(jnp.bfloat16)
    partial_value = jnp.dot(hidden, down_weight, preferred_element_type=jnp.float32)
    grad_hidden = contract_cols(dy_full, down_weight)
    grad_gate_pre = (grad_hidden * up_pre * slope).astype(jnp.bfloat16)
    grad_up_pre = (grad_hidden * active).astype(jnp.bfloat16)
    input_partial = contract_cols(grad_gate_pre, gate_weight) + contract_cols(
        grad_up_pre, up_weight
    )
    out_piece, input_piece = reduce_pieces(
        [partial_value.astype(jnp.bfloat16), input_partial.astype(jnp.bfloat16)], 1
    )
    hidden_in, gate_in, up_in, out_piece, input_piece = lax.optimization_barrier(
        (hidden, grad_gate_pre, grad_up_pre, out_piece, input_piece)
    )
    hidden_blocks, gate_blocks, up_blocks = gather([hidden_in, gate_in, up_in], 2)
    out_back = lax.all_to_all(
        out_piece.reshape(groups, capacity, piece_width),
        "ep",
        split_axis=0,
        concat_axis=0,
        tiled=True,
    ).reshape(buffer_rows, piece_width)
    out_tokens = (
        jnp.take(out_back, slot_index, axis=0)
        .reshape(tok_rows, chosen, piece_width)
        .astype(jnp.float32)
    )
    mixed = jnp.sum(combine_weights[:, :, None] * out_tokens, axis=1).astype(jnp.bfloat16)
    local_products = jnp.sum(cotangent.astype(jnp.float32)[:, None, :] * out_tokens, axis=2)
    grad_combine = lax.psum(local_products, "tp")
    input_back = lax.all_to_all(
        input_piece.reshape(groups, capacity, piece_width),
        "ep",
        split_axis=0,
        concat_axis=0,
        tiled=True,
    ).reshape(buffer_rows, piece_width)
    grad_tokens = jnp.sum(
        jnp.take(input_back, slot_index, axis=0)
        .reshape(tok_rows, chosen, piece_width)
        .astype(jnp.float32),
        axis=1,
    ).astype(jnp.bfloat16)
    down_cols_out = (
        jnp.einsum("nrh,rd->nhd", hidden_blocks, recv_grad, preferred_element_type=jnp.float32)
        .astype(jnp.bfloat16)
        .reshape(-1, piece_width)
    )
    x_turned = recv_rows.T
    gate_rows_out = row_grads(x_turned, gate_blocks)
    up_rows_out = row_grads(x_turned, up_blocks)
    return (
        mixed,
        grad_tokens,
        grad_combine,
        gate_rows_out[None],
        up_rows_out[None],
        down_cols_out[None],
    )


def solution(mesh):
    placed = (
        P("ep", "tp"),
        P("ep", "tp"),
        P("ep", None),
        P("ep", None),
        P("ep", None, "tp"),
        P("ep", None, "tp"),
        P("ep", "tp", None),
    )
    return jax.shard_map(
        body,
        mesh=mesh,
        in_specs=placed,
        out_specs=(
            P("ep", "tp"),
            P("ep", "tp"),
            P("ep", None),
            P("ep", "tp", None),
            P("ep", "tp", None),
            P("ep", None, "tp"),
        ),
        check_vma=False,
    )
```
